32 devices in a mesh: lat: 4 (over z), lon: 4 (over y, x), fold: 2 (over core).
Axes of the slice: x: 2, y: 2, z: 4, core: 2. Of those that a mesh axis runs over, the one named last changes fastest.
Arguments:
- field: float32 [2, 12, 640, 2560], P('fold', None, 'lat', 'lon'), may hold values from -6 to 6
- row_shift: int32 [2, 12, 640, 2560], P('fold', None, 'lat', 'lon'), may hold values from -4 to 4
- col_shift: int32 [2, 12, 640, 2560], P('fold', None, 'lat', 'lon'), may hold values from -4 to 4
- row_frac: bfloat16 [2, 12, 640, 2560], P('fold', None, 'lat', 'lon'), may hold values from 0 to 1
- col_frac: bfloat16 [2, 12, 640, 2560], P('fold', None, 'lat', 'lon'), may hold values from 0 to 1
- wave_map: int32 [16], replicated, may hold values from 0 to 1279, as said below
- legendre: float32 [16, 640, 1280], P('lon', 'lat'), may hold values from -0.25 to 0.25
- helm_coef: float32 [12], P('fold'), may hold values from 1e-06 to 0.0001
Outputs:
- spectrum: float32 [12, 4, 4, 2560], P('fold', 'lon', 'lat')
The draws below stay inside these ranges and needn't reach their ends.
Inputs may be any that keep to these rules, and one draw needn't show every extreme that they name: `col_shift`: longitude offset of the departure cell. `wave_map`: distinct zonal wavenumbers.
All inputs are finite; a program needn't handle non-finite values.
Results may differ from the reference program's by a relative error of at most 0.0003.
Values sent between devices are 32-bit elements; how exact they have to be, the bound alone decides.
A program may use at most 64 MiB of HBM per device.

```python
import math
import jax
import jax.numpy as jnp
from jax import lax

LAT_HALF = 640
LON_CELLS = 2560
DEGREES = 1280
SHIFT_MAX = 4
LEVEL_DEV = 12
GROUPS = 2
LEVELS = 12
WAVES_LON = 4
WAVE_SLOTS = 16
N_LON = 4


def draw_wave_map(key, part):
    ordering = jax.random.permutation(key, DEGREES)
    return ordering[:WAVE_SLOTS].astype(jnp.int32)


def plant(result, key, least, largest):
    shape = result.shape
    index_at = [jax.random.randint(jax.random.fold_in(key, axis), (), 0, shape[axis]) for axis in range(len(shape))]
    result = result.at[tuple(index_at)].set(least)
    longest = shape.index(max(shape))
    index_at[longest] = (index_at[longest] + 1) % shape[longest]
    return result.at[tuple(index_at)].set(largest)


def level_of(key, extent, split, smallest, top_value):
    def one(dim, blocks):
        steps = jax.random.uniform(jax.random.fold_in(jax.random.fold_in(key, 6), dim), (blocks,), jnp.float32, smallest / len(split), top_value / len(split))
        return jnp.repeat(jnp.exp(steps), extent[dim] // blocks).reshape((-1,) + (1,) * (len(extent) - dim - 1))

    level = one(*split[0])
    for cut in split[1:]:
        level = level * one(*cut)
    return level


def gaussian(stream_key, dims, scale, bound, pieces=(), held_as=jnp.bfloat16):
    factor_of = level_of(stream_key, dims, pieces, -0.22, 0.18) if pieces else 1.0
    drawn = jax.random.normal(stream_key, dims, jnp.float32) * scale * factor_of
    return jnp.minimum(jnp.maximum(drawn, -bound), bound).astype(held_as)


def setup_inputs(seed: int = 0) -> dict:
    seeds = jax.random.split(jax.random.key(seed), 9)
    return {
        "field": gaussian(seeds[0], (GROUPS, LEVEL_DEV, LAT_HALF, LON_CELLS), 1.0, 6.0, ((0, 2), (2, 4), (3, 4)), jnp.float32),
        "row_shift": plant(jax.random.randint(seeds[1], (GROUPS, LEVEL_DEV, LAT_HALF, LON_CELLS), 0 - SHIFT_MAX, SHIFT_MAX + 1), jax.random.fold_in(seeds[1], 1), 0 - SHIFT_MAX, SHIFT_MAX).astype(jnp.int32),
        "col_shift": plant(jax.random.randint(seeds[2], (GROUPS, LEVEL_DEV, LAT_HALF, LON_CELLS), 0 - SHIFT_MAX, SHIFT_MAX + 1), jax.random.fold_in(seeds[2], 1), 0 - SHIFT_MAX, SHIFT_MAX).astype(jnp.int32),
        "row_frac": jnp.clip(1.0 * jax.random.uniform(seeds[3], (GROUPS, LEVEL_DEV, LAT_HALF, LON_CELLS), jnp.float32) ** level_of(seeds[3], (GROUPS, LEVEL_DEV, LAT_HALF, LON_CELLS), ((0, 2), (2, 4), (3, 4)), -0.2, 0.2), 0.0, 1.0).astype(jnp.bfloat16),
        "col_frac": jnp.clip(1.0 * jax.random.uniform(seeds[4], (GROUPS, LEVEL_DEV, LAT_HALF, LON_CELLS), jnp.float32) ** level_of(seeds[4], (GROUPS, LEVEL_DEV, LAT_HALF, LON_CELLS), ((0, 2), (2, 4), (3, 4)), -0.2, 0.2), 0.0, 1.0).astype(jnp.bfloat16),
        "wave_map": draw_wave_map(jax.random.fold_in(seeds[8], 71), 0),
        "legendre": gaussian(seeds[6], (WAVE_SLOTS, LAT_HALF, DEGREES), LAT_HALF ** -0.5, 0.25, ((0, 4), (1, 4)), jnp.float32),
        "helm_coef": jnp.clip(jnp.exp(math.log(0.0001) - 4.6051702 * jax.random.uniform(seeds[7], (LEVELS,), jnp.float32) ** level_of(seeds[7], (LEVELS,), ((0, 2),), -0.2, 0.2)), 9.999999974752427e-07, 0.0001),
    }


def cubic_weights(fraction):
    return (-fraction * (fraction - 1.0) * (fraction - 2.0) / 6.0, (fraction + 1.0) * (fraction - 1.0) * (fraction - 2.0) / 2.0, -(fraction + 1.0) * fraction * (fraction - 2.0) / 2.0, (fraction + 1.0) * fraction * (fraction - 1.0) / 6.0)

def interpolate(padded, row_shift, col_shift, row_frac, col_frac, margin):
    levels, rows, cols = row_shift.shape
    width = cols + 2 * margin
    flat = padded.reshape(levels, -1)
    row_base = lax.broadcasted_iota(jnp.int32, (levels, rows, cols), 1) + row_shift + (margin - 1)
    col_base = lax.broadcasted_iota(jnp.int32, (levels, rows, cols), 2) + col_shift + (margin - 1)
    start_index = (row_base * width + col_base).reshape(levels, -1).astype(jnp.int32)
    row_weights = cubic_weights(row_frac.astype(jnp.float32).reshape(levels, -1))
    col_weights = cubic_weights(col_frac.astype(jnp.float32).reshape(levels, -1))
    total = jnp.zeros(start_index.shape, jnp.float32)
    for row_step in range(4):
        line = jnp.zeros(start_index.shape, jnp.float32)
        for col_step in range(4):
            taken = jnp.take_along_axis(flat, start_index + (row_step * width + col_step), axis=1)
            line = line + col_weights[col_step] * taken
        total = total + row_weights[row_step] * line
    return total.reshape(levels, rows, cols)

def zonal_table(waves, first_col, count_cols, lon_total):
    col_ids = first_col + lax.iota(jnp.int32, count_cols)
    phase = col_ids[:, None] * waves[None, :] % lon_total
    angle = phase.astype(jnp.float32) * (2.0 * math.pi / lon_total)
    return jnp.stack([jnp.cos(angle), -jnp.sin(angle)], axis=1) / math.sqrt(lon_total)

def reference(field, row_shift, col_shift, row_frac, col_frac, wave_map, legendre, helm_coef):
    margin = SHIFT_MAX + 2
    blocks = GROUPS // 2
    fields = field.reshape(blocks, 2, LEVEL_DEV, LAT_HALF, LON_CELLS)
    opposite = fields[:, ::-1]
    band = opposite[:, :, :, ::-1, :][:, :, :, :margin, :]
    polar = jnp.zeros((blocks, 2, LEVEL_DEV, margin, LON_CELLS), jnp.float32)
    extended = jnp.concatenate([polar, fields, band], axis=3)
    extended = jnp.concatenate([extended[..., -margin:], extended, extended[..., :margin]], axis=4)
    number = blocks * 2 * LEVEL_DEV

    def one_field(items):
        padded, shift_rows, shift_cols, frac_rows, frac_cols = items
        return interpolate(padded[None], shift_rows[None], shift_cols[None], frac_rows[None], frac_cols[None], margin)[0]
    gridded = lax.map(one_field, (extended.reshape(number, LAT_HALF + 2 * margin, LON_CELLS + 2 * margin), row_shift.reshape(number, LAT_HALF, LON_CELLS), col_shift.reshape(number, LAT_HALF, LON_CELLS), row_frac.reshape(number, LAT_HALF, LON_CELLS), col_frac.reshape(number, LAT_HALF, LON_CELLS)))
    gridded = gridded.reshape(blocks, 2, LEVEL_DEV, LAT_HALF, LON_CELLS)
    even = (gridded[:, 0] + gridded[:, 1]).reshape(LEVELS, LAT_HALF, LON_CELLS)
    odd = (gridded[:, 0] - gridded[:, 1]).reshape(LEVELS, LAT_HALF, LON_CELLS)
    table = zonal_table(wave_map, 0, LON_CELLS, LON_CELLS)
    zonal_even = jnp.einsum('lkx,xqs->lsqk', even, table, precision=lax.Precision.HIGHEST)
    zonal_odd = jnp.einsum('lkx,xqs->lsqk', odd, table, precision=lax.Precision.HIGHEST)
    sum_even = jnp.einsum('lsqk,skn->lsqn', zonal_even, legendre, precision=lax.Precision.HIGHEST)
    sum_odd = jnp.einsum('lsqk,skn->lsqn', zonal_odd, legendre, precision=lax.Precision.HIGHEST)
    degrees = jnp.arange(DEGREES, dtype=jnp.int32)
    parity = (wave_map[:, None] + degrees[None, :]) % 2 == 0
    keep = (degrees[None, :] >= wave_map[:, None]).astype(jnp.float32)
    legendre_sum = jnp.where(parity[None, :, None, :], sum_even, sum_odd) * keep[None, :, None, :]
    degree_float = degrees.astype(jnp.float32)
    damping = 1.0 + helm_coef[:, None, None, None] * (degree_float * (degree_float + 1.0))[None, None, None, :]
    spectrum = legendre_sum / damping
    return spectrum.reshape(LEVELS, N_LON, WAVES_LON, 2 * DEGREES)
```

```python
import functools
import math

import jax
import jax.numpy as jnp
from jax import lax
from jax.experimental import pallas as pl
from jax.experimental.pallas import tpu as pltpu
from jax.sharding import PartitionSpec as P

SHIFT_MAX = 4
LANES = 128
HEAD = 8


def cubic_weights(t):
    tm, tp, td = t - 1.0, t + 1.0, t - 2.0
    outer = t * tm
    inner = tp * td
    return (
        outer * (td * (-1.0 / 6.0)),
        inner * (tm * 0.5),
        inner * (t * -0.5),
        outer * (tp * (1.0 / 6.0)),
    )


def tiles_of(cols, margin):
    usable = LANES - 2 * margin + 1
    count = -(-cols // usable)
    stride = -(-cols // count)
    tiles = []
    for t in range(count):
        low, high = t * stride, min(cols, (t + 1) * stride)
        start = min(low, cols - LANES)
        base = margin - 1 if start == low else -margin
        tiles.append((start, base, low, high))
    return tiles


def interp_kernel(
    tiles,
    margin,
    field,
    north,
    south,
    west,
    east,
    row_shift,
    col_shift,
    row_frac,
    col_frac,
    table,
    out,
    source,
    row_t,
    col_t,
    grid,
):
    rows, cols = field.shape[1:]
    row_t[...] = row_frac[0].astype(jnp.float32)
    col_t[...] = col_frac[0].astype(jnp.float32)
    for t, (start, base, _, _) in enumerate(tiles):
        first = start - base
        lead = max(0, -first)
        trail = max(0, first + LANES - cols)
        mid_a, mid_b = first + lead, first + LANES - trail
        a, b = lead, LANES - trail
        source[t, HEAD - margin : HEAD, a:b] = north[0, :, mid_a:mid_b]
        source[t, HEAD : HEAD + rows, a:b] = field[0, :, mid_a:mid_b]
        source[t, HEAD + rows : HEAD + rows + margin, a:b] = south[0, :, mid_a:mid_b]
        span = rows + 2 * margin
        if lead:
            source[t, HEAD - margin : HEAD - margin + span, 0:lead] = west[0, :, margin - lead :]
        if trail:
            source[t, HEAD - margin : HEAD - margin + span, b:LANES] = east[0, :, :trail]

    lane = lax.broadcasted_iota(jnp.int32, (8, LANES), 1)
    blocks = rows // 8
    unroll = next(u for u in (5, 4, 3, 2, 1) if blocks % u == 0)
    window = range(1 - margin, margin + 1)

    for t, (start, base, _, _) in enumerate(tiles):
        low = -base + (margin - 1)
        high = LANES - 1 - base - margin
        place = jnp.clip(lane, low, high) + (base - 1)
        floor, shift = start // LANES * LANES, start % LANES

        def read(ref, at):
            if shift == 0:
                return ref[at, floor : floor + LANES]
            pair = ref[at, floor : floor + 2 * LANES]
            return pltpu.roll(pair, 2 * LANES - shift, 1)[:, :LANES]

        def one(j):
            at = pl.ds(pl.multiple_of(8 * j, 8), 8)
            cs = read(col_shift.at[0], at)
            rs = read(row_shift.at[0], at)
            wc = cubic_weights(read(col_t, at))
            wr = cubic_weights(read(row_t, at))
            origin = place + cs
            index = [origin + step for step in range(4)]
            lines = []
            for offset in window:
                cells = source[t, pl.ds(8 * j + (HEAD + offset), 8), :]
                line = None
                for step in range(4):
                    taken = jnp.take_along_axis(
                        cells, index[step], axis=1, mode="promise_in_bounds"
                    )
                    term = wc[step] * taken
                    line = term if line is None else line + term
                lines.append(line)
            left = rs + SHIFT_MAX
            reach = SHIFT_MAX
            while reach >= 1:
                far = left >= reach + (1 if reach > 1 else 0)
                count = len(lines) - reach
                lines = [jnp.where(far, lines[i + reach], lines[i]) for i in range(count)]
                left = jnp.where(far, left - reach, left)
                if reach == 1:
                    break
                reach //= 2
            far = left >= 1
            if len(lines) > 4:
                lines = [jnp.where(far, lines[i + 1], lines[i]) for i in range(4)]
            total = wr[0] * lines[0]
            for step in range(1, 4):
                total = total + wr[step] * lines[step]
            grid[at, t * LANES : (t + 1) * LANES] = total

        def body(outer, carry):
            for k in range(unroll):
                one(outer * unroll + k)
            return carry

        lax.fori_loop(0, blocks // unroll, body, 0)

    half = table.shape[1] // 2
    values = grid[...]
    top = values.astype(jnp.bfloat16)
    rest = (values - top.astype(jnp.float32)).astype(jnp.bfloat16)
    both = jnp.dot(top, table[...], preferred_element_type=jnp.float32)
    more = jnp.dot(rest, table[:, :half], preferred_element_type=jnp.float32)
    out[0] = (both[:, :half] + both[:, half:] + more).T


def interpolated_waves(field, halos, shifts, fracs, table, tiles, margin):
    levels, rows, cols = field.shape
    north, south, west, east = halos

    def whole(x):
        return pl.BlockSpec((1,) + x.shape[1:], lambda i: (i, 0, 0))

    operands = [field, north, south, west, east, *shifts, *fracs]
    half = table.shape[1] // 2
    return pl.pallas_call(
        functools.partial(interp_kernel, tiles, margin),
        grid=(levels,),
        in_specs=[whole(x) for x in operands]
        + [pl.BlockSpec(table.shape, lambda i: (0, 0))],
        out_specs=pl.BlockSpec((1, half, rows), lambda i: (i, 0, 0)),
        out_shape=jax.ShapeDtypeStruct((levels, half, rows), jnp.float32),
        scratch_shapes=[
            pltpu.VMEM((len(tiles), rows + 16, LANES), jnp.float32),
            pltpu.VMEM((rows, cols), jnp.float32),
            pltpu.VMEM((rows, cols), jnp.float32),
            pltpu.VMEM((rows, len(tiles) * LANES), jnp.float32),
        ],
    )(*operands, table)


def zonal_table(waves, first_col, tiles, lon_total):
    lane = lax.broadcasted_iota(jnp.int32, (len(tiles), LANES), 1)
    starts = jnp.array([t[0] for t in tiles], jnp.int32)[:, None]
    lows = jnp.array([t[2] for t in tiles], jnp.int32)[:, None]
    highs = jnp.array([t[3] for t in tiles], jnp.int32)[:, None]
    local_col = lane + starts
    own = ((local_col >= lows) & (local_col < highs)).reshape(-1)
    col = (first_col + local_col).reshape(-1)
    phase = waves[:, None] * col[None, :] % lon_total
    angle = phase.astype(jnp.float32) * (2.0 * math.pi / lon_total)
    pair = jnp.stack([jnp.cos(angle), -jnp.sin(angle)], axis=1) / math.sqrt(lon_total)
    pair = jnp.where(own, pair, 0.0)
    full = pair.reshape(-1, pair.shape[-1])
    top = full.astype(jnp.bfloat16)
    rest = (full - lax.reduce_precision(full, 8, 7)).astype(jnp.bfloat16)
    return jnp.concatenate([top, rest], axis=0).T


def halos_of(grid, margin):
    rows, cols = grid.shape[1:]
    n_lat, n_fold, n_lon = (lax.axis_size(a) for a in ("lat", "fold", "lon"))
    place = lax.axis_index("lat")
    head, tail = grid[:, :margin], grid[:, rows - margin :]
    north = lax.ppermute(tail, "lat", [(i, i + 1) for i in range(n_lat - 1)])
    below = lax.ppermute(head, "lat", [(i + 1, i) for i in range(n_lat - 1)])
    last = n_lat - 1
    mirror = lax.ppermute(
        tail[:, ::-1],
        ("lat", "fold"),
        [(last * n_fold + f, last * n_fold + (f ^ 1)) for f in range(n_fold)],
    )
    south = jnp.where(place == last, mirror, below)

    def edge(a, b):
        return jnp.concatenate([north[:, :, a:b], grid[:, :, a:b], south[:, :, a:b]], axis=1)

    west = lax.ppermute(
        edge(cols - margin, cols), "lon", [(i, (i + 1) % n_lon) for i in range(n_lon)]
    )
    east = lax.ppermute(edge(0, margin), "lon", [((i + 1) % n_lon, i) for i in range(n_lon)])
    return north, south, west, east


def local(field, row_shift, col_shift, row_frac, col_frac, wave_map, legendre, helm_coef):
    margin = SHIFT_MAX + 2
    grid = field[0]
    levels, rows, cols = grid.shape
    half = levels // 2
    n_lon, n_lat, n_fold = (lax.axis_size(a) for a in ("lon", "lat", "fold"))
    lon_total = cols * n_lon
    lon_place = lax.axis_index("lon")
    tiles = tiles_of(cols, margin)
    table = zonal_table(wave_map, lon_place * cols, tiles, lon_total)
    waves_here = interpolated_waves(
        grid,
        halos_of(grid, margin),
        (row_shift[0], col_shift[0]),
        (row_frac[0], col_frac[0]),
        table,
        tiles,
        margin,
    )
    slots = wave_map.shape[0]
    slots_here = slots // n_lon
    hemisphere = lax.axis_index("fold") % 2
    sign = (1 - 2 * hemisphere).astype(jnp.float32)
    by_slot = jnp.transpose(waves_here.reshape(levels, slots, 2, rows), (1, 2, 0, 3))
    coeffs = lax.psum_scatter(by_slot, "lon", scatter_dimension=0, tiled=True)
    outgoing = lax.dynamic_slice_in_dim(coeffs, (1 - hemisphere) * half, half, 2)
    incoming = lax.ppermute(outgoing, "fold", [(f, f ^ 1) for f in range(n_fold)])
    kept = lax.dynamic_slice_in_dim(coeffs, hemisphere * half, half, 2)
    folded = jnp.stack([kept + incoming, sign * (kept - incoming)], axis=2)
    degree_count = legendre.shape[2]
    degrees = lax.iota(jnp.int32, degree_count)
    waves = lax.dynamic_slice_in_dim(wave_map, lon_place * slots_here, slots_here)
    product = jnp.einsum("sqelk,skn->selqn", folded, legendre, precision=lax.Precision.HIGHEST)
    parity = (waves[:, None] + degrees[None, :]) % 2 == 0
    keep = degrees[None, :] >= waves[:, None]
    picked = jnp.where(parity[:, None, None, :], product[:, 0], product[:, 1])
    picked = jnp.where(keep[:, None, None, :], picked, 0.0)
    summed = lax.psum_scatter(
        picked.reshape(slots_here, half, 2 * degree_count), "lat", scatter_dimension=0, tiled=True
    )
    degree_float = degrees.astype(jnp.float32)
    pair = jnp.concatenate([degree_float, degree_float])
    damping = 1.0 + helm_coef[None, :, None] * (pair * (pair + 1.0))[None, None, :]
    return jnp.transpose(summed / damping, (1, 0, 2))[:, None, :, :]


def solution(mesh):
    block = P("fold", None, "lat", "lon")
    in_specs = (block,) * 5 + (P(), P("lon", "lat", None), P("fold"))
    out_specs = P("fold", "lon", "lat", None)
    return jax.shard_map(local, mesh=mesh, in_specs=in_specs, out_specs=out_specs, check_vma=False)
```

```python
import functools
import math

import jax
import jax.numpy as jnp
from jax import lax
from jax.experimental import pallas as pl
from jax.experimental.pallas import tpu as pltpu
from jax.sharding import PartitionSpec as P

SHIFT_MAX = 4
LANES = 128
HEAD = 8


def cubic_weights(t):
    tm, tp, td = t - 1.0, t + 1.0, t - 2.0
    outer = t * tm
    inner = tp * td
    return (
        outer * (td * (-1.0 / 6.0)),
        inner * (tm * 0.5),
        inner * (t * -0.5),
        outer * (tp * (1.0 / 6.0)),
    )


def interp_kernel(
    margin,
    last,
    field,
    north,
    below,
    mirror,
    west,
    east,
    row_shift,
    col_shift,
    row_frac,
    col_frac,
    table,
    out,
    padded,
    source,
    row_t,
    col_t,
    grid,
):
    rows, cols = field.shape[1:]
    count = cols // LANES
    span = rows + 2 * HEAD
    row_t[...] = row_frac[0].astype(jnp.float32)
    col_t[...] = col_frac[0].astype(jnp.float32)
    inner = slice(LANES, LANES + cols)
    padded[0:HEAD, inner] = north[0]
    padded[HEAD : HEAD + rows, inner] = field[0]
    at_last = jnp.full((1, cols), last[0], jnp.int32) == 1
    for i in range(HEAD):
        line = jnp.where(at_last, mirror[0, HEAD - 1 - i : HEAD - i], below[0, i : i + 1])
        padded[HEAD + rows + i : HEAD + rows + i + 1, inner] = line
    padded[:, LANES - HEAD : LANES] = west[0].T
    padded[:, LANES + cols : LANES + cols + HEAD] = east[0].T

    lane = lax.broadcasted_iota(jnp.int32, (span, LANES), 1)
    for c in range(2 * margin):
        move = c + 1 - margin
        side = (move > 0) - (move < 0)
        near = [
            padded[:, (t + 1) * LANES : (t + 2) * LANES]
            for t in range(min(0, side), count + max(0, side))
        ]
        if side:
            near = [pltpu.roll(x, -move % LANES, 1) for x in near]
        for t in range(count):
            if side > 0:
                source[c, t] = jnp.where(lane < LANES - move, near[t], near[t + 1])
            elif side < 0:
                source[c, t] = jnp.where(lane >= -move, near[t + 1], near[t])
            else:
                source[c, t] = near[t]

    blocks = rows // 8
    unroll = next(u for u in (2, 1) if blocks % u == 0)
    window = range(1 - margin, margin + 1)

    for t in range(count):

        def read(ref, at):
            return ref[at, t * LANES : (t + 1) * LANES]

        def one(j):
            at = pl.ds(pl.multiple_of(8 * j, 8), 8)
            cs = read(col_shift.at[0], at)
            rs = read(row_shift.at[0], at)
            wc = cubic_weights(read(col_t, at))
            wr = cubic_weights(read(row_t, at))
            lines = [None] * len(window)
            hits = [cs == v for v in range(-SHIFT_MAX, SHIFT_MAX + 1)]
            spread = []
            for place_at in range(len(window)):
                w = None
                for step in range(4):
                    v = place_at - step
                    if 0 <= v < len(hits):
                        w = jnp.where(hits[v], wc[step], 0.0 if w is None else w)
                spread.append(w)
            for slot, offset in enumerate(window):
                for c in range(len(window)):
                    cells = source[c, t, pl.ds(8 * j + (HEAD + offset), 8), :]
                    term = spread[c] * cells
                    lines[slot] = term if c == 0 else lines[slot] + term
            left = rs + SHIFT_MAX
            reach = SHIFT_MAX
            while reach >= 1:
                far = left >= reach + (1 if reach > 1 else 0)
                taps = len(lines) - reach
                lines = [jnp.where(far, lines[i + reach], lines[i]) for i in range(taps)]
                left = jnp.where(far, left - reach, left)
                if reach == 1:
                    break
                reach //= 2
            far = left >= 1
            if len(lines) > 4:
                lines = [jnp.where(far, lines[i + 1], lines[i]) for i in range(4)]
            total = wr[0] * lines[0]
            for step in range(1, 4):
                total = total + wr[step] * lines[step]
            grid[at, t * LANES : (t + 1) * LANES] = total

        def body(outer, carry):
            for k in range(unroll):
                one(outer * unroll + k)
            return carry

        lax.fori_loop(0, blocks // unroll, body, 0)

    half = table.shape[1] // 2
    values = grid[...]
    top = values.astype(jnp.bfloat16)
    rest = (values - top.astype(jnp.float32)).astype(jnp.bfloat16)
    both = jnp.dot(top, table[...], preferred_element_type=jnp.float32)
    more = jnp.dot(rest, table[:, :half], preferred_element_type=jnp.float32)
    sums = both[:, :half] + both[:, half:] + more
    out[0] = sums.T.reshape(out.shape[1:])


def interpolated_waves(field, halos, shifts, fracs, table, last, n_lon, margin):
    levels, rows, cols = field.shape

    def whole(x):
        return pl.BlockSpec((1,) + x.shape[1:], lambda i: (i, 0, 0))

    operands = [field, *halos, *shifts, *fracs]
    shape = (levels, n_lon, table.shape[1] // 2 // n_lon, rows)
    return pl.pallas_call(
        functools.partial(interp_kernel, margin),
        grid=(levels,),
        in_specs=[pl.BlockSpec(memory_space=pltpu.SMEM)]
        + [whole(x) for x in operands]
        + [pl.BlockSpec(table.shape, lambda i: (0, 0))],
        out_specs=pl.BlockSpec((1,) + shape[1:], lambda i: (i, 0, 0, 0)),
        out_shape=jax.ShapeDtypeStruct(shape, jnp.float32),
        scratch_shapes=[
            pltpu.VMEM((rows + 2 * HEAD, cols + 2 * LANES), jnp.float32),
            pltpu.VMEM((2 * margin, cols // LANES, rows + 2 * HEAD, LANES), jnp.float32),
            pltpu.VMEM((rows, cols), jnp.float32),
            pltpu.VMEM((rows, cols), jnp.float32),
            pltpu.VMEM((rows, cols), jnp.float32),
        ],
    )(last, *operands, table)


def zonal_table(waves, first_col, cols, lon_total):
    col = first_col + lax.iota(jnp.int32, cols)
    phase = waves[:, None] * col[None, :] % lon_total
    angle = phase.astype(jnp.float32) * (2.0 * math.pi / lon_total)
    pair = jnp.stack([jnp.cos(angle), -jnp.sin(angle)], axis=1) / math.sqrt(lon_total)
    full = pair.reshape(-1, cols)
    top = full.astype(jnp.bfloat16)
    rest = (full - lax.reduce_precision(full, 8, 7)).astype(jnp.bfloat16)
    return jnp.concatenate([top, rest], axis=0).T


def halos_of(grid):
    rows, cols = grid.shape[1:]
    n_lat, n_fold, n_lon = (lax.axis_size(a) for a in ("lat", "fold", "lon"))
    last = n_lat - 1
    at_last = lax.axis_index("lat") == last
    head, tail = grid[:, :HEAD], grid[:, rows - HEAD :]
    north = lax.ppermute(tail, "lat", [(i, i + 1) for i in range(last)])
    below = lax.ppermute(head, "lat", [(i + 1, i) for i in range(last)])
    route = [(last * n_fold + f, last * n_fold + (f ^ 1)) for f in range(n_fold)]
    mirror = lax.ppermute(tail, ("lat", "fold"), route)

    def edge(a, b):
        south = jnp.where(at_last, mirror[:, ::-1, a:b], below[:, :, a:b])
        strip = jnp.concatenate([north[:, :, a:b], grid[:, :, a:b], south], axis=1)
        return jnp.swapaxes(strip, 1, 2)

    ring = [(i, (i + 1) % n_lon) for i in range(n_lon)]
    west = lax.ppermute(edge(cols - HEAD, cols), "lon", ring)
    east = lax.ppermute(edge(0, HEAD), "lon", [(b, a) for a, b in ring])
    return at_last.astype(jnp.int32).reshape(1), (north, below, mirror, west, east)


def scatter_sum(pieces, axis):
    count = lax.axis_size(axis)
    place = lax.axis_index(axis)
    total = lax.dynamic_index_in_dim(pieces, place, 0, keepdims=False)
    arrived = []
    for step in range(1, count):
        piece = lax.dynamic_index_in_dim(pieces, (place + step) % count, 0, keepdims=False)
        arrived.append(lax.ppermute(piece, axis, [(i, (i + step) % count) for i in range(count)]))
    for part in arrived:
        total = total + part
    return total


def local(field, row_shift, col_shift, row_frac, col_frac, wave_map, legendre, helm_coef):
    margin = SHIFT_MAX + 2
    grid = field[0]
    levels, rows, cols = grid.shape
    half = levels // 2
    n_lon, n_lat, n_fold = (lax.axis_size(a) for a in ("lon", "lat", "fold"))
    lon_place = lax.axis_index("lon")
    table = zonal_table(wave_map, lon_place * cols, cols, cols * n_lon)
    last, halos = halos_of(grid)
    waves_here = interpolated_waves(
        grid,
        halos,
        (row_shift[0], col_shift[0]),
        (row_frac[0], col_frac[0]),
        table,
        last,
        n_lon,
        margin,
    )
    slots_here = wave_map.shape[0] // n_lon
    hemisphere = lax.axis_index("fold") % 2
    sign = (1 - 2 * hemisphere).astype(jnp.float32)
    coeffs = scatter_sum(jnp.swapaxes(waves_here, 0, 1), "lon")
    outgoing = lax.dynamic_slice_in_dim(coeffs, (1 - hemisphere) * half, half, 0)
    incoming = lax.ppermute(outgoing, "fold", [(f, f ^ 1) for f in range(n_fold)])
    kept = lax.dynamic_slice_in_dim(coeffs, hemisphere * half, half, 0)
    folded = jnp.stack([kept + incoming, sign * (kept - incoming)], axis=0)
    folded = jnp.transpose(folded.reshape(2, half, slots_here, 2, rows), (2, 3, 0, 1, 4))
    degree_count = legendre.shape[2]
    degrees = lax.iota(jnp.int32, degree_count)
    waves = lax.dynamic_slice_in_dim(wave_map, lon_place * slots_here, slots_here)
    product = jnp.einsum("sqelk,skn->selqn", folded, legendre, precision=lax.Precision.HIGHEST)
    parity = (waves[:, None] + degrees[None, :]) % 2 == 0
    keep = degrees[None, :] >= waves[:, None]
    picked = jnp.where(parity[:, None, None, :], product[:, 0], product[:, 1])
    picked = jnp.where(keep[:, None, None, :], picked, 0.0)
    summed = scatter_sum(
        picked.reshape(n_lat, slots_here // n_lat, half, 2 * degree_count), "lat"
    )
    degree_float = degrees.astype(jnp.float32)
    pair = jnp.concatenate([degree_float, degree_float])
    damping = 1.0 + helm_coef[None, :, None] * (pair * (pair + 1.0))[None, None, :]
    return jnp.transpose(summed / damping, (1, 0, 2))[:, None, :, :]


def solution(mesh):
    block = P("fold", None, "lat", "lon")
    in_specs = (block,) * 5 + (P(), P("lon", "lat", None), P("fold"))
    out_specs = P("fold", "lon", "lat", None)
    return jax.shard_map(local, mesh=mesh, in_specs=in_specs, out_specs=out_specs, check_vma=False)
```
